16 devices in a mesh: dp: 2 (over y, z), tp: 8 (over x, core).
Axes of the slice: x: 4, y: 2, z: 1, core: 2. Of those that a mesh axis runs over, the one named last changes fastest.
The devices are a block of a 4x4x8 slice.
Arguments:
- x: bfloat16 [4096, 4096], P('dp'), parts along dimension 0
- mu1: float32 [4096], P('dp'), parts along dimension 0
- rs1: float32 [4096], P('dp'), parts along dimension 0
- g1: bfloat16 [4096], replicated
- g2: bfloat16 [4096], replicated
- dy: bfloat16 [4096, 4096], P('dp'), parts along dimension 0
- wqkv: bfloat16 [4096, 12288], P(None, 'tp')
- wo: bfloat16 [32, 128, 4096], P('tp')
- w1: bfloat16 [4096, 16384], P(None, 'tp')
- w2: bfloat16 [16384, 4096], P('tp')
Outputs:
- output 1: bfloat16 [4096, 4096], P('dp'), parts along dimension 0
- output 2: bfloat16 [8192, 12288], P('dp', 'tp'), parts along dimension 0
- output 3: bfloat16 [64, 128, 4096], P(('dp', 'tp')), parts along dimension 0
- output 4: bfloat16 [8192, 16384], P('dp', 'tp'), parts along dimension 0
- output 5: bfloat16 [32768, 4096], P(('dp', 'tp')), parts along dimension 0
There are 2 independent parts. The reference program is written for one: setup_inputs(seed, part) draws one part's arguments, and reference() takes and returns one part's arrays. A program takes and returns all parts, laid end to end along the dimension named above; an argument that names none is the same for every part.
All inputs are finite; a program needn't handle non-finite values.
Results may differ from the reference program's by a relative error of at most 0.016693.
Values are sent between devices in bfloat16 or wider.
A program may use at most 768 MiB of HBM per device.

```python
import jax
import jax.numpy as jnp
from jax import lax

T = 2048
D = 4096
HEADS = 32
FF = 16384
HEAD = D // HEADS
EPS = 1.0 / 100000
QK_GAIN = 2.5 ** 0.5


def setup_inputs(seed: int = 0, part: int = 0) -> dict:
    kp = jax.random.fold_in(jax.random.key(seed), part)
    ka = jax.random.split(kp, 4)
    kw = jax.random.split(jax.random.key(seed + 1), 6)
    z = jax.random.normal(ka[0], (T, D), jnp.float32)
    z = z - jnp.mean(z, axis=-1, keepdims=True)
    z = z * lax.rsqrt(jnp.mean(z * z, axis=-1, keepdims=True))
    mu1 = 0.5 * jax.random.normal(ka[1], (T,), jnp.float32)
    rs1 = jax.random.uniform(ka[2], (T,), jnp.float32, 0.7, 1.4)
    x = (mu1[:, None] + z / rs1[:, None]).astype(jnp.bfloat16)
    dy = jax.random.normal(ka[3], (T, D), jnp.float32).astype(jnp.bfloat16)
    g1 = jax.random.uniform(kw[0], (D,), jnp.float32, 0.6, 1.4).astype(jnp.bfloat16)
    g2 = jax.random.uniform(kw[1], (D,), jnp.float32, 0.6, 1.4).astype(jnp.bfloat16)
    gain = jnp.array([QK_GAIN, QK_GAIN, 1.0], jnp.float32)[None, None, :, None]
    wqkv = jax.random.normal(kw[2], (D, HEADS, 3, HEAD), jnp.float32) * gain * D ** -0.5
    wo = jax.random.normal(kw[3], (HEADS, HEAD, D), jnp.float32) * D ** -0.5
    w1 = jax.random.normal(kw[4], (D, FF), jnp.float32) * D ** -0.5
    w2 = jax.random.normal(kw[5], (FF, D), jnp.float32) * FF ** -0.5
    return {"x": x, "mu1": mu1, "rs1": rs1, "g1": g1, "g2": g2, "dy": dy,
            "wqkv": wqkv.reshape(D, 3 * D).astype(jnp.bfloat16), "wo": wo.astype(jnp.bfloat16),
            "w1": w1.astype(jnp.bfloat16), "w2": w2.astype(jnp.bfloat16)}


def _ln_bwd(dn, xh, rs, g):
    u = dn * g
    return rs[:, None] * (u - jnp.mean(u, axis=-1, keepdims=True) - xh * jnp.mean(u * xh, axis=-1, keepdims=True))


def _probs(q, k):
    s = jnp.dot(q, k.T, preferred_element_type=jnp.float32) * HEAD ** -0.5
    mask = jnp.arange(T)[:, None] >= jnp.arange(T)[None, :]
    return jax.nn.softmax(jnp.where(mask, s, -jnp.inf), axis=-1)


def _head_fwd(qkv):
    q, k, v = qkv[:, 0], qkv[:, 1], qkv[:, 2]
    p = _probs(q, k)
    return jnp.dot(p.astype(jnp.bfloat16), v, preferred_element_type=jnp.float32).astype(jnp.bfloat16)


def _head_bwd(args):
    qkv, do = args
    q, k, v = qkv[:, 0], qkv[:, 1], qkv[:, 2]
    p = _probs(q, k)
    dv = jnp.dot(p.astype(jnp.bfloat16).T, do, preferred_element_type=jnp.float32)
    dpm = jnp.dot(do, v.T, preferred_element_type=jnp.float32)
    ds = (p * (dpm - jnp.sum(p * dpm, axis=-1, keepdims=True)) * HEAD ** -0.5).astype(jnp.bfloat16)
    dq = jnp.dot(ds, k, preferred_element_type=jnp.float32)
    dk = jnp.dot(ds.T, q, preferred_element_type=jnp.float32)
    return jnp.stack([dq, dk, dv], axis=1).astype(jnp.bfloat16)


def reference(x, mu1, rs1, g1, g2, dy, wqkv, wo, w1, w2):
    xf = x.astype(jnp.float32)
    g1f = g1.astype(jnp.float32)
    g2f = g2.astype(jnp.float32)
    xh1 = (xf - mu1[:, None]) * rs1[:, None]
    n1 = (xh1 * g1f).astype(jnp.bfloat16)
    qkv = jnp.dot(n1, wqkv, preferred_element_type=jnp.float32).astype(jnp.bfloat16)
    qkv = jnp.moveaxis(qkv.reshape(T, HEADS, 3, HEAD), 1, 0)
    o = lax.map(_head_fwd, qkv)
    o = jnp.moveaxis(o, 0, 1).reshape(T, D)
    wo2 = wo.reshape(D, D)
    h1 = xf + jnp.dot(o, wo2, preferred_element_type=jnp.float32)
    mu2 = jnp.mean(h1, axis=-1, keepdims=True)
    xc = h1 - mu2
    rs2 = lax.rsqrt(jnp.mean(xc * xc, axis=-1) + EPS)
    xh2 = xc * rs2[:, None]
    n2 = (xh2 * g2f).astype(jnp.bfloat16)
    a = jnp.dot(n2, w1, preferred_element_type=jnp.float32)
    gl, gelu_vjp = jax.vjp(jax.nn.gelu, a)
    gb = gl.astype(jnp.bfloat16)
    dw2 = jnp.dot(gb.T, dy, preferred_element_type=jnp.float32).astype(jnp.bfloat16)
    dg = jnp.dot(dy, w2.T, preferred_element_type=jnp.float32)
    da = gelu_vjp(dg)[0].astype(jnp.bfloat16)
    dw1 = jnp.dot(n2.T, da, preferred_element_type=jnp.float32).astype(jnp.bfloat16)
    dn2 = jnp.dot(da, w1.T, preferred_element_type=jnp.float32)
    dh1 = dy.astype(jnp.float32) + _ln_bwd(dn2, xh2, rs2, g2f)
    dh1b = dh1.astype(jnp.bfloat16)
    dwo = jnp.dot(o.T, dh1b, preferred_element_type=jnp.float32).astype(jnp.bfloat16).reshape(HEADS, HEAD, D)
    do = jnp.dot(dh1b, wo2.T, preferred_element_type=jnp.float32).astype(jnp.bfloat16)
    do = jnp.moveaxis(do.reshape(T, HEADS, HEAD), 1, 0)
    dqkv = lax.map(_head_bwd, (qkv, do))
    dqkv = jnp.moveaxis(dqkv, 0, 1).reshape(T, 3 * D)
    dwqkv = jnp.dot(n1.T, dqkv, preferred_element_type=jnp.float32).astype(jnp.bfloat16)
    dn1 = jnp.dot(dqkv, wqkv.T, preferred_element_type=jnp.float32)
    dx = (dh1 + _ln_bwd(dn1, xh1, rs1, g1f)).astype(jnp.bfloat16)
    return dx, dwqkv, dwo, dw1, dw2
```

```python
import functools

import jax
import jax.numpy as jnp
from jax import lax
from jax.experimental import pallas as pl
from jax.experimental.pallas import tpu as pltpu
from jax.sharding import PartitionSpec as P

EPS = 1.0 / 100000
F32 = jnp.float32
BF = jnp.bfloat16
NC = 2
BQ = 512


def _ln_bwd(dn, xh, rs, g):
    u = dn * g
    return rs * (u - jnp.mean(u, axis=-1, keepdims=True) - xh * jnp.mean(u * xh, axis=-1, keepdims=True))


def _nt(a, b):
    return lax.dot_general(a, b, (((1,), (1,)), ((), ())), preferred_element_type=F32)


def _tn(a, b):
    return lax.dot_general(a, b, (((0,), (0,)), ((), ())), preferred_element_type=F32)


def _nn(a, b):
    return jnp.dot(a, b, preferred_element_type=F32)


def _attn_fwd_kernel(chunk, *refs):
    qkv, o_ref = refs[:-1], refs[-1]
    hd = o_ref.shape[1]
    rows = o_ref.shape[0]
    scale = hd ** -0.5
    bq = min(BQ, rows)
    for b in range(rows // bq):
        q = qkv[chunk][b * bq:(b + 1) * bq, 0:hd]
        parts = [(c, rows) for c in range(chunk)] + [(chunk, (b + 1) * bq)]
        s = [_nt(q, qkv[c][0:n, hd:2 * hd]) for c, n in parts]
        n = (b + 1) * bq
        row = b * bq + lax.broadcasted_iota(jnp.int32, (bq, n), 0)
        col = lax.broadcasted_iota(jnp.int32, (bq, n), 1)
        s[-1] = jnp.where(row >= col, s[-1], -jnp.inf)
        m = functools.reduce(jnp.maximum, [jnp.max(x, axis=-1, keepdims=True) for x in s])
        p = [jnp.exp((x - m) * scale) for x in s]
        l = functools.reduce(jnp.add, [jnp.sum(x, axis=-1, keepdims=True) for x in p])
        inv = 1.0 / l
        o = None
        for x, (c, n) in zip(p, parts):
            t = _nn((x * inv).astype(BF), qkv[c][0:n, 2 * hd:3 * hd])
            o = t if o is None else o + t
        o_ref[b * bq:(b + 1) * bq, :] = o.astype(BF)


def _attn_fwd(chunk, qkvs, hl, hd):
    rows = qkvs[0].shape[0]
    pairs = rows * rows * chunk + rows * rows // 2
    return pl.pallas_call(
        functools.partial(_attn_fwd_kernel, chunk),
        grid=(hl,),
        in_specs=[pl.BlockSpec((rows, 3 * hd), lambda h: (0, h)) for _ in range(chunk + 1)],
        out_specs=pl.BlockSpec((rows, hd), lambda h: (0, h)),
        out_shape=jax.ShapeDtypeStruct((rows, hl * hd), BF),
        compiler_params=pltpu.CompilerParams(vmem_limit_bytes=60 * 2 ** 20),
        cost_estimate=pl.CostEstimate(flops=8 * hl * pairs * hd, bytes_accessed=rows * hl * hd * 8 * (chunk + 1), transcendentals=hl * pairs),
        name=f"attn_fwd_{chunk}",
    )(*qkvs[:chunk + 1])


def _attn_bwd_kernel(chunk, nc, *refs):
    qkv, refs = refs[:chunk + 1], refs[chunk + 1:]
    do_ref, refs = refs[0], refs[1:]
    late = chunk < nc - 1
    prev, refs = (refs[:2], refs[2:]) if late else (None, refs)
    out_ref, refs = refs[0], refs[1:]
    part = refs[:2 * chunk]
    acc_k, acc_v = refs[2 * chunk:]
    hd = do_ref.shape[1]
    rows = do_ref.shape[0]
    scale = hd ** -0.5
    bq = min(BQ, rows)
    for b in range(rows // bq):
        sl = slice(b * bq, (b + 1) * bq)
        q = qkv[chunk][sl, 0:hd]
        do = do_ref[sl, :]
        parts = [(c, rows) for c in range(chunk)] + [(chunk, (b + 1) * bq)]
        s = [_nt(qkv[c][0:n, hd:2 * hd], q) for c, n in parts]
        n = (b + 1) * bq
        key = lax.broadcasted_iota(jnp.int32, (n, bq), 0)
        qry = b * bq + lax.broadcasted_iota(jnp.int32, (n, bq), 1)
        s[-1] = jnp.where(qry >= key, s[-1], -jnp.inf)
        m = functools.reduce(jnp.maximum, [jnp.max(x, axis=0, keepdims=True) for x in s])
        p = [jnp.exp((x - m) * scale) for x in s]
        inv = 1.0 / functools.reduce(jnp.add, [jnp.sum(x, axis=0, keepdims=True) for x in p])
        p = [x * inv for x in p]
        dp = [_nt(qkv[c][0:n, 2 * hd:3 * hd], do) for c, n in parts]
        r = functools.reduce(jnp.add, [jnp.sum(x * y, axis=0, keepdims=True) for x, y in zip(p, dp)])
        dq = None
        for x, y, (c, n) in zip(p, dp, parts):
            ds = (x * (y - r) * scale).astype(BF)
            dv = _nn(x.astype(BF), do)
            dk = _nn(ds, q)
            t = _tn(ds, qkv[c][0:n, hd:2 * hd])
            dq = t if dq is None else dq + t
            if c == chunk:
                if b == 0:
                    acc_k[0:n, :] = prev[0][0:n, :] + dk if late else dk
                    acc_v[0:n, :] = prev[1][0:n, :] + dv if late else dv
                else:
                    lo = b * bq
                    acc_k[0:lo, :] = acc_k[0:lo, :] + dk[0:lo]
                    acc_v[0:lo, :] = acc_v[0:lo, :] + dv[0:lo]
                    acc_k[lo:n, :] = prev[0][lo:n, :] + dk[lo:n] if late else dk[lo:n]
                    acc_v[lo:n, :] = prev[1][lo:n, :] + dv[lo:n] if late else dv[lo:n]
            elif b == 0:
                part[2 * c][...] = dk
                part[2 * c + 1][...] = dv
            else:
                part[2 * c][...] = part[2 * c][...] + dk
                part[2 * c + 1][...] = part[2 * c + 1][...] + dv
        out_ref[sl, 0:hd] = dq.astype(BF)
    out_ref[:, hd:2 * hd] = acc_k[...].astype(BF)
    out_ref[:, 2 * hd:3 * hd] = acc_v[...].astype(BF)


def _attn_bwd(chunk, nc, qkvs, do, prev, hl, hd):
    rows = do.shape[0]
    pairs = rows * rows * chunk + rows * rows // 2
    wide = pl.BlockSpec((rows, 3 * hd), lambda h: (0, h))
    one = pl.BlockSpec((rows, hd), lambda h: (0, h))
    res = pl.pallas_call(
        functools.partial(_attn_bwd_kernel, chunk, nc),
        grid=(hl,),
        in_specs=[wide] * (chunk + 1) + [one] + [one] * len(prev),
        out_specs=[wide] + [one] * (2 * chunk),
        out_shape=[jax.ShapeDtypeStruct((rows, 3 * hl * hd), BF)]
        + [jax.ShapeDtypeStruct((rows, hl * hd), F32)] * (2 * chunk),
        scratch_shapes=[pltpu.VMEM((rows, hd), F32), pltpu.VMEM((rows, hd), F32)],
        compiler_params=pltpu.CompilerParams(vmem_limit_bytes=62 * 2 ** 20),
        cost_estimate=pl.CostEstimate(flops=20 * hl * pairs * hd, bytes_accessed=rows * hl * hd * 8 * (chunk + 2), transcendentals=hl * pairs),
        name=f"attn_bwd_{chunk}",
    )(*qkvs[:chunk + 1], do, *prev)
    return res[0], list(res[1:])


MESH = pl.DeviceIdType.MESH
VMEM = 62 * 2 ** 20
C0 = 0.7978845608028654
C1 = 0.044715


def _dot(a, b, ta, tb):
    return lax.dot_general(a, b, (((0 if ta else 1,), (1 if tb else 0,)), ((), ())), preferred_element_type=F32)


def _norm_qkv_kernel(x_ref, mu_ref, rs_ref, g_ref, w_ref, n_ref, o_ref):
    xh = (x_ref[...].astype(F32) - mu_ref[...]) * rs_ref[...]
    n_ref[...] = (xh * g_ref[...]).astype(BF)
    o_ref[...] = _nn(n_ref[...], w_ref[...]).astype(BF)


def _norm_qkv(x, mu, rs, g, w, lo, rows):
    bm = 256
    d, n = w.shape
    off = lo // bm
    return pl.pallas_call(
        _norm_qkv_kernel,
        grid=(rows // bm,),
        in_specs=[pl.BlockSpec((bm, d), lambda i: (i + off, 0)),
                  pl.BlockSpec((bm, 1), lambda i: (i + off, 0)),
                  pl.BlockSpec((bm, 1), lambda i: (i + off, 0)),
                  pl.BlockSpec((1, d), lambda i: (0, 0)),
                  pl.BlockSpec((d, n), lambda i: (0, 0))],
        out_specs=[pl.BlockSpec((bm, d), lambda i: (i, 0)), pl.BlockSpec((bm, n), lambda i: (i, 0))],
        out_shape=[jax.ShapeDtypeStruct((rows, d), BF), jax.ShapeDtypeStruct((rows, n), BF)],
        compiler_params=pltpu.CompilerParams(vmem_limit_bytes=VMEM),
        cost_estimate=pl.CostEstimate(flops=2 * rows * d * n, bytes_accessed=2 * (2 * rows * d + d * n + rows * n), transcendentals=0),
        name="norm_qkv",
    )(x, mu, rs, g, w)


def _gather_events(step, marks, shard, out, local, ssem, rsem):
    tp = lax.axis_size("tp")
    me = lax.axis_index("tp")
    chips = tp // 2
    chip, core = me // 2, lax.rem(me, 2)
    sr = shard.shape[0]
    h = sr // 2

    def dev(shift, other=0):
        k = 1 - core if other else core
        return lax.rem(chip + shift, chips) * 2 + k

    right, left, opp, mate = dev(1), dev(chips - 1), dev(2), dev(0, 1)

    def rows(owner, part=None):
        if part is None:
            return out.at[pl.ds(pl.multiple_of(owner * sr, 8), sr)]
        return out.at[pl.ds(pl.multiple_of(owner * sr + part * h, 8), h)]

    def copy(i, src, dst, to):
        return pltpu.make_async_remote_copy(src_ref=src, dst_ref=dst, send_sem=ssem.at[i], recv_sem=rsem.at[i],
                                            device_id={"tp": to}, device_id_type=MESH)

    lo, hi = shard.at[pl.ds(0, h)], shard.at[pl.ds(h, h)]
    sends = [copy(0, lo, rows(me, 0), right), copy(1, hi, rows(me, 1), left),
             copy(2, hi, rows(me, 1), right), copy(3, lo, rows(me, 0), left),
             copy(4, shard, rows(me), mate),
             copy(5, rows(left, 0), rows(left, 0), right), copy(6, rows(right, 1), rows(right, 1), left),
             copy(7, rows(left), rows(left), mate), copy(8, rows(right), rows(right), mate),
             copy(9, rows(opp), rows(opp), mate)]
    lands = [rows(left, 0), rows(right, 1), rows(left, 1), rows(right, 0), rows(mate), rows(opp, 0), rows(opp, 1),
             rows(dev(chips - 1, 1)), rows(dev(1, 1)), rows(dev(2, 1))]

    def landed(i):
        copy(i, lands[i], lands[i], mate).wait_recv()

    own = pltpu.make_async_copy(shard, rows(me), local)

    @pl.when(step == 0)
    def _():
        bar = pltpu.get_barrier_semaphore()
        for to in (left, right, mate):
            pl.semaphore_signal(bar, inc=1, device_id={"tp": to}, device_id_type=MESH)
        pl.semaphore_wait(bar, 3)
        for i in range(5):
            sends[i].start()
        own.start()

    @pl.when(step == marks[0])
    def _():
        landed(0)
        sends[5].start()
        landed(1)
        sends[6].start()

    @pl.when(step == marks[1])
    def _():
        landed(2)
        sends[7].start()
        landed(3)
        sends[8].start()

    def finish():
        landed(5)
        landed(6)
        sends[9].start()
        for i in (4, 7, 8, 9):
            landed(i)
        own.wait()
        for cp in sends:
            cp.wait_send()

    return finish


def _mm(body, grid, ins, in_specs, outs, out_specs, flops, name, shard=None, cid=0, marks=(0, 0)):
    n_in, n_out = len(ins), len(outs)
    steps = grid[0] * grid[1]

    def plain(*refs):
        body(refs[:n_in], refs[n_in:])

    def comm(*refs):
        sh, out = refs[n_in], refs[n_in + 1 + n_out]
        step = pl.program_id(0) * grid[1] + pl.program_id(1)
        finish = _gather_events(step, marks, sh, out, *refs[n_in + n_out + 2:])
        body(refs[:n_in], refs[n_in + 1:n_in + 1 + n_out])
        pl.when(step == steps - 1)(finish)

    nbytes = sum(v.size * v.dtype.itemsize for v in ins) + sum(v.size * v.dtype.itemsize for v in outs)
    cost = pl.CostEstimate(flops=flops, bytes_accessed=nbytes, transcendentals=0)
    if shard is None:
        return pl.pallas_call(plain, grid=grid, in_specs=in_specs, out_specs=out_specs, out_shape=outs, cost_estimate=cost,
                              compiler_params=pltpu.CompilerParams(vmem_limit_bytes=VMEM), name=name)(*ins)
    any_spec = pl.BlockSpec(memory_space=pl.ANY)
    full = jax.ShapeDtypeStruct((shard.shape[0] * lax.axis_size("tp"), shard.shape[1]), shard.dtype)
    return pl.pallas_call(
        comm, grid=grid, in_specs=in_specs + [any_spec], out_specs=out_specs + [any_spec], out_shape=outs + [full],
        scratch_shapes=[pltpu.SemaphoreType.DMA, pltpu.SemaphoreType.DMA((10,)), pltpu.SemaphoreType.DMA((10,))],
        cost_estimate=cost, name=name,
        compiler_params=pltpu.CompilerParams(vmem_limit_bytes=VMEM, collective_id=cid, has_side_effects=True))(*ins, shard)


def _matmul(a, b, tb, bm, bn, name, dtype=BF, **kw):
    m, k = a.shape
    n = b.shape[0] if tb else b.shape[1]

    def body(i, o):
        o[0][...] = _dot(i[0][...], i[1][...], False, tb).astype(dtype)

    return _mm(body, (m // bm, n // bn), [a, b],
               [pl.BlockSpec((bm, k), lambda i, j: (i, 0)),
                pl.BlockSpec((bn, k), lambda i, j: (j, 0)) if tb else pl.BlockSpec((k, bn), lambda i, j: (0, j))],
               [jax.ShapeDtypeStruct((m, n), dtype)], [pl.BlockSpec((bm, bn), lambda i, j: (i, j))],
               2 * m * n * k, name, **kw)


def _mlp_up(n2, dg, w, lo, bn=512, sub=256, **kw):
    m, k = n2.shape
    n = w.shape[1]
    off = lo // m

    def body(i, o):
        for s in range(0, bn, sub):
            sl = slice(s, s + sub)
            a = _nn(i[0][...], i[1][:, sl])
            a2 = a * a
            th = jnp.tanh(C0 * a * (1.0 + C1 * a2))
            p1 = 0.5 + 0.5 * th
            o[0][:, sl] = (a * p1).astype(BF)
            der = p1 + (a * (0.5 * C0)) * (1.0 - th * th) * (1.0 + (3.0 * C1) * a2)
            o[1][:, sl] = (i[2][:, sl] * der).astype(BF)

    tile = pl.BlockSpec((m, bn), lambda i, j: (i, j))
    return _mm(body, (1, n // bn), [n2, w, dg],
               [pl.BlockSpec((m, k), lambda i, j: (0, 0)), pl.BlockSpec((k, bn), lambda i, j: (0, j)),
                pl.BlockSpec((m, bn), lambda i, j: (off, j))],
               [jax.ShapeDtypeStruct((m, n), BF)] * 2, [tile, tile], 2 * m * n * k, "mlp_up", **kw)


def _wgrad(lhs, rhs, bm, bn, name, **kw):
    rows = min(v.shape[0] for v in lhs + rhs)

    def pieces(vs, width, pick):
        arrays, specs = [], []
        for v in vs:
            for p in range(v.shape[0] // rows):
                arrays.append(v)
                specs.append(pl.BlockSpec((rows, width), functools.partial(lambda p, i, j: (p, pick(i, j)), p)))
        return arrays, specs

    la, ls = pieces(lhs, bm, lambda i, j: i)
    ra, rs = pieces(rhs, bn, lambda i, j: j)
    n = len(la)
    m, w = lhs[0].shape[1], rhs[0].shape[1]

    def body(i, o):
        acc = _dot(i[0][...], i[n][...], True, False)
        for e in range(1, n):
            acc += _dot(i[e][...], i[n + e][...], True, False)
        o[0][...] = acc.astype(BF)

    return _mm(body, (m // bm, w // bn), la + ra, ls + rs, [jax.ShapeDtypeStruct((m, w), BF)],
               [pl.BlockSpec((bm, bn), lambda i, j: (i, j))], 2 * m * w * rows * n, name, **kw)


def solution(mesh):
    tp = mesh.shape["tp"]

    def body(x, mu1, rs1, g1, g2, dy, wqkv, wo, w1, w2):
        hl, hd, d = wo.shape
        t = x.shape[0]
        ct = t // NC
        sh = ct // tp
        me = lax.axis_index("tp")
        wo2 = wo.reshape(hl * hd, d)
        g1f = g1.astype(F32)
        g2f = g2.astype(F32)
        muc, rsc, g1r = mu1[:, None], rs1[:, None], g1f[None, :]

        def rows(v, c):
            return lax.dynamic_slice_in_dim(v, c * ct + me * sh, sh, 0)

        def rscat(v):
            return lax.psum_scatter(v, "tp", scatter_dimension=0, tiled=True)

        def gather(v):
            return lax.all_gather(v, "tp", axis=0, tiled=True)

        def after(v, dep):
            return lax.optimization_barrier((v, dep))[0]

        def ln2(c, red):
            h1 = rows(x, c).astype(F32) + red.astype(F32)
            xc = h1 - jnp.mean(h1, axis=-1, keepdims=True)
            rs2 = lax.rsqrt(jnp.mean(xc * xc, axis=-1, keepdims=True) + EPS)
            xh2 = xc * rs2
            return (xh2 * g2f).astype(BF), xh2, rs2

        def fwd(c, x):
            n1, qkv = _norm_qkv(x, muc, rsc, g1r, wqkv, c * ct, ct)
            qkvs.append(qkv)
            n1s.append(n1)
            os.append(_attn_fwd(c, qkvs, hl, hd))
            return _matmul(os[c], wo2, False, ct, 1024, "attn_out")[0]

        n1s, qkvs, os = [], [], []
        p0 = fwd(0, x)
        r0 = rscat(p0)
        p1 = fwd(1, after(x, p0))
        r1 = rscat(p1)
        n2a, xh2a, rs2a = ln2(0, after(r0, p1))
        dg, n2_0 = _matmul(dy, w2, True, 1024, 512, "dgate", F32, shard=n2a, cid=0, marks=(3, 5))
        gb0, da0 = _mlp_up(n2_0, dg, w1, 0)
        n2b, xh2b, rs2b = ln2(1, after(r1, da0))
        q0, n2_1 = _matmul(da0, w1, True, ct, 512, "mlp_back", shard=n2b, cid=1, marks=(5, 7))
        s0 = rscat(q0)
        gb1, da1 = _mlp_up(after(n2_1, q0), dg, w1, ct)
        q1 = _matmul(da1, w1, True, ct, 512, "mlp_back")[0]
        s1 = rscat(q1)
        dw2 = _wgrad([gb0, after(gb1, q1)], [dy], 1024, 1024, "dw2")[0]

        def dln2(c, red, xh2, rs2):
            v = rows(dy, c).astype(F32) + _ln_bwd(red.astype(F32), xh2, rs2, g2f)
            return v, v.astype(BF)

        dh1a, dha = dln2(0, after(s0, dw2), xh2a, rs2a)
        dh1b, dhb = dln2(1, after(s1, dha), xh2b, rs2b)
        dh1_1 = gather(dhb)
        dh1_0 = gather(after(dha, dhb))
        dw1 = _wgrad([n2_0, n2_1], [da0, after(da1, dhb)], 1024, 1024, "dw1")[0]

        def bwd(c, dh, prev):
            do = _matmul(dh, wo2, True, 512, hl * hd, "dattn_out")[0]
            dqkv, prev = _attn_bwd(c, NC, qkvs, do, prev, hl, hd)
            return dqkv, prev, _matmul(dqkv, wqkv, True, ct, 512, "qkv_back")[0]

        dqkv1, prev, u1 = bwd(1, after(dh1_1, dw1), [])
        v1 = rscat(u1)
        dqkv0, prev, u0 = bwd(0, after(dh1_0, u1), prev)
        v0 = rscat(u0)

        def dln1(c, red, dh1):
            xh1 = (rows(x, c).astype(F32) - rows(muc, c)) * rows(rsc, c)
            return (dh1 + _ln_bwd(red.astype(F32), xh1, rows(rsc, c), g1f)).astype(BF)

        dwqkv = _wgrad(n1s, [after(dqkv0, u0), dqkv1], 1024, dqkv0.shape[1] // 2, "dwqkv")[0]
        dwo = _wgrad(os, [after(dh1_0, u0), dh1_1], hl * hd, 1024, "dwo")[0]
        dxb = dln1(1, after(v1, dwqkv), dh1b)
        dxa = dln1(0, after(v0, dxb), dh1a)
        dx = lax.all_gather(jnp.stack([dxa, dxb], 0), "tp", axis=1, tiled=True).reshape(t, d)
        return dx, dwqkv, dwo.reshape(hl, hd, d), dw1, dw2

    return jax.shard_map(
        body, mesh=mesh,
        in_specs=(P("dp", None), P("dp"), P("dp"), P(None), P(None), P("dp", None),
                  P(None, "tp"), P("tp", None, None), P(None, "tp"), P("tp", None)),
        out_specs=(P("dp", None), P("dp", "tp"), P(("dp", "tp"), None, None), P("dp", "tp"), P(("dp", "tp"), None)),
        check_vma=False)
```

```python
import functools

import jax
import jax.numpy as jnp
from jax import lax
from jax.experimental import pallas as pl
from jax.experimental.pallas import tpu as pltpu
from jax.sharding import PartitionSpec as P

EPS = 1.0 / 100000
F32 = jnp.float32
BF = jnp.bfloat16
NC = 2
BQ = 256
ROWS = 32
LOG2E = 1.4426950408889634


def _mean(x):
    return jnp.mean(x, axis=-1, keepdims=True)


def _ln_bwd(dn, xh, rs, g):
    u = dn * g
    return rs * (u - _mean(u) - xh * _mean(u * xh))


def _nt(a, b):
    return lax.dot_general(a, b, (((1,), (1,)), ((), ())), preferred_element_type=F32)


def _tn(a, b):
    return lax.dot_general(a, b, (((0,), (0,)), ((), ())), preferred_element_type=F32)


def _nn(a, b):
    return jnp.dot(a, b, preferred_element_type=F32)


def _max(x, axis):
    return jnp.max(x, axis=axis, keepdims=True)


def _sum(x, axis):
    return jnp.sum(x, axis=axis, keepdims=True)


def _total(xs):
    return functools.reduce(jnp.add, xs)


def _columns(hd):
    return [slice(e * hd, (e + 1) * hd) for e in range(3)]


def _parts(chunk, rows, b, bq):
    lo = b * bq
    parts = [(c, slice(0, rows)) for c in range(chunk)]
    if b:
        parts.append((chunk, slice(0, lo)))
    return parts + [(chunk, slice(lo, lo + bq))]


def _attn_fwd_kernel(chunk, *refs):
    qkv, o_ref = refs[:-1], refs[-1]
    rows, hd = o_ref.shape
    qc, kc, vc = _columns(hd)
    scale = hd ** -0.5 * LOG2E
    bq = min(BQ, rows)
    mask = lax.broadcasted_iota(jnp.int32, (bq, bq), 0) >= lax.broadcasted_iota(jnp.int32, (bq, bq), 1)
    for b in range(rows // bq):
        parts = _parts(chunk, rows, b, bq)
        me = parts[-1][1]
        q = qkv[chunk][me, qc]
        s = [_nt(q, qkv[c][sl, kc]) for c, sl in parts]
        s[-1] = jnp.where(mask, s[-1], -jnp.inf)
        m = functools.reduce(jnp.maximum, [_max(x, -1) for x in s]) * scale
        p = [jnp.exp2(x * scale - m) for x in s]
        inv = 1.0 / _total([_sum(x, -1) for x in p])
        o = _total([_nn(x.astype(BF), qkv[c][sl, vc]) for x, (c, sl) in zip(p, parts)])
        o_ref[me, :] = (o * inv).astype(BF)


def _attn_fwd(chunk, qkvs, hl, hd):
    rows = qkvs[0].shape[0]
    pairs = rows * rows * chunk + rows * rows // 2
    return pl.pallas_call(
        functools.partial(_attn_fwd_kernel, chunk),
        grid=(hl,),
        in_specs=[pl.BlockSpec((rows, 3 * hd), lambda h: (0, h)) for _ in range(chunk + 1)],
        out_specs=pl.BlockSpec((rows, hd), lambda h: (0, h)),
        out_shape=jax.ShapeDtypeStruct((rows, hl * hd), BF),
        compiler_params=pltpu.CompilerParams(vmem_limit_bytes=60 * 2 ** 20),
        cost_estimate=pl.CostEstimate(flops=8 * hl * pairs * hd, bytes_accessed=rows * hl * hd * 8 * (chunk + 1), transcendentals=hl * pairs),
        name=f"attn_fwd_{chunk}",
    )(*qkvs[:chunk + 1])


def _attn_bwd_kernel(chunk, late, *refs):
    qkv, do_ref, refs = refs[:chunk + 1], refs[chunk + 1], list(refs[chunk + 2:])
    prev = (refs.pop(0), refs.pop(0)) if late else ()
    out_ref = refs.pop(0)
    sums = [(refs.pop(0), refs.pop(0)) for _ in range(chunk + 1)]
    rows, hd = do_ref.shape
    qc, kc, vc = _columns(hd)
    scale = hd ** -0.5
    bq = min(BQ, rows)
    mask = lax.broadcasted_iota(jnp.int32, (bq, bq), 1) >= lax.broadcasted_iota(jnp.int32, (bq, bq), 0)
    for b in range(rows // bq):
        parts = _parts(chunk, rows, b, bq)
        me = parts[-1][1]
        q = qkv[chunk][me, qc]
        do = do_ref[me, :]
        s = [_nt(qkv[c][sl, kc], q) for c, sl in parts]
        s[-1] = jnp.where(mask, s[-1], -jnp.inf)
        m = functools.reduce(jnp.maximum, [_max(x, 0) for x in s]) * (scale * LOG2E)
        p = [jnp.exp2(x * (scale * LOG2E) - m) for x in s]
        inv = 1.0 / _total([_sum(x, 0) for x in p])
        p = [x * inv for x in p]
        dp = [_nt(qkv[c][sl, vc], do) for c, sl in parts]
        r = _total([_sum(x * y, 0) for x, y in zip(p, dp)])
        dq = []
        for x, y, (c, sl) in zip(p, dp, parts):
            ds = (x * (y - r)).astype(BF)
            new = (_nn(ds, q), _nn(x.astype(BF), do))
            dq.append(_tn(ds, qkv[c][sl, kc]))
            fresh = sl is me if c == chunk else b == 0
            for e, (acc, v) in enumerate(zip(sums[c], new)):
                if not fresh:
                    v += acc[sl, :]
                elif c == chunk and late:
                    v += prev[e][sl, :]
                acc[sl, :] = v
        out_ref[me, qc] = (_total(dq) * scale).astype(BF)
    acc_k, acc_v = sums[chunk]
    out_ref[:, kc] = (acc_k[...] * scale).astype(BF)
    out_ref[:, vc] = acc_v[...].astype(BF)


def _attn_bwd(chunk, nc, qkvs, do, prev, hl, hd):
    rows = do.shape[0]
    pairs = rows * rows * chunk + rows * rows // 2
    wide = pl.BlockSpec((rows, 3 * hd), lambda h: (0, h))
    one = pl.BlockSpec((rows, hd), lambda h: (0, h))
    res = pl.pallas_call(
        functools.partial(_attn_bwd_kernel, chunk, chunk < nc - 1),
        grid=(hl,),
        in_specs=[wide] * (chunk + 1) + [one] + [one] * len(prev),
        out_specs=[wide] + [one] * (2 * chunk),
        out_shape=[jax.ShapeDtypeStruct((rows, 3 * hl * hd), BF)]
        + [jax.ShapeDtypeStruct((rows, hl * hd), F32)] * (2 * chunk),
        scratch_shapes=[pltpu.VMEM((rows, hd), F32), pltpu.VMEM((rows, hd), F32)],
        compiler_params=pltpu.CompilerParams(vmem_limit_bytes=62 * 2 ** 20),
        cost_estimate=pl.CostEstimate(flops=20 * hl * pairs * hd, bytes_accessed=rows * hl * hd * 8 * (chunk + 2), transcendentals=hl * pairs),
        name=f"attn_bwd_{chunk}",
    )(*qkvs[:chunk + 1], do, *prev)
    return res[0], list(res[1:])


MESH = pl.DeviceIdType.MESH
VMEM = 62 * 2 ** 20
C0 = 0.7978845608028654
C1 = 0.044715


def _dot(a, b, ta, tb):
    return lax.dot_general(a, b, (((0 if ta else 1,), (1 if tb else 0,)), ((), ())), preferred_element_type=F32)


def _column(v):
    return jnp.transpose(jnp.broadcast_to(v, (128, v.shape[1])))[:, :1]


def _norm_qkv_kernel(x_ref, mu_ref, rs_ref, g_ref, w_ref, n_ref, o_ref):
    xh = (x_ref[...].astype(F32) - _column(mu_ref[...])) * _column(rs_ref[...])
    n_ref[...] = (xh * g_ref[...]).astype(BF)
    o_ref[...] = _nn(n_ref[...], w_ref[...]).astype(BF)


def _norm_qkv(x, mu, rs, g, w, lo, rows):
    bm = 256
    d, n = w.shape
    off = lo // bm
    return pl.pallas_call(
        _norm_qkv_kernel,
        grid=(rows // bm,),
        in_specs=[pl.BlockSpec((bm, d), lambda i: (i + off, 0)),
                  pl.BlockSpec((1, bm), lambda i: (0, i + off)),
                  pl.BlockSpec((1, bm), lambda i: (0, i + off)),
                  pl.BlockSpec((1, d), lambda i: (0, 0)),
                  pl.BlockSpec((d, n), lambda i: (0, 0))],
        out_specs=[pl.BlockSpec((bm, d), lambda i: (i, 0)), pl.BlockSpec((bm, n), lambda i: (i, 0))],
        out_shape=[jax.ShapeDtypeStruct((rows, d), BF), jax.ShapeDtypeStruct((rows, n), BF)],
        compiler_params=pltpu.CompilerParams(vmem_limit_bytes=VMEM),
        cost_estimate=pl.CostEstimate(flops=2 * rows * d * n, bytes_accessed=2 * (2 * rows * d + d * n + rows * n), transcendentals=0),
        name="norm_qkv",
    )(x, mu, rs, g, w)


def _gather_plan(shard, out, local, ssem, rsem):
    tp = lax.axis_size("tp")
    me = lax.axis_index("tp")
    chips = tp // 2
    chip, core = me // 2, lax.rem(me, 2)
    sr = shard.shape[0]
    h = sr // 2

    def dev(shift, other=0):
        k = 1 - core if other else core
        return lax.rem(chip + shift, chips) * 2 + k

    right, left, opp, mate = dev(1), dev(chips - 1), dev(2), dev(0, 1)

    def rows(owner, part=None):
        if part is None:
            return out.at[pl.ds(pl.multiple_of(owner * sr, 8), sr)]
        return out.at[pl.ds(pl.multiple_of(owner * sr + part * h, 8), h)]

    def copy(i, src, dst, to):
        return pltpu.make_async_remote_copy(src_ref=src, dst_ref=dst, send_sem=ssem.at[i], recv_sem=rsem.at[i],
                                            device_id={"tp": to}, device_id_type=MESH)

    lo, hi = shard.at[pl.ds(0, h)], shard.at[pl.ds(h, h)]
    moves = [(lo, rows(me, 0), right), (hi, rows(me, 1), left), (hi, rows(me, 1), right), (lo, rows(me, 0), left), (shard, rows(me), mate)]
    for v, to in ((rows(left, 0), right), (rows(right, 1), left), (rows(left), mate), (rows(right), mate), (rows(opp), mate)):
        moves.append((v, v, to))
    sends = [copy(i, *move) for i, move in enumerate(moves)]
    lands = [rows(left, 0), rows(right, 1), rows(left, 1), rows(right, 0), rows(mate), rows(opp, 0), rows(opp, 1),
             rows(dev(chips - 1, 1)), rows(dev(1, 1)), rows(dev(2, 1))]

    def landed(i):
        copy(i, lands[i], lands[i], mate).wait_recv()

    own = pltpu.make_async_copy(shard, rows(me), local)

    def begin():
        for i in range(5):
            sends[i].start()
        own.start()

    def forward():
        landed(0)
        sends[5].start()
        landed(1)
        sends[6].start()

    def share():
        landed(2)
        sends[7].start()
        landed(3)
        sends[8].start()

    def finish():
        landed(5)
        landed(6)
        sends[9].start()
        for i in (4, 7, 8, 9):
            landed(i)
        own.wait()
        for cp in sends:
            cp.wait_send()

    return (left, right, mate), begin, forward, share, finish


def _gather_events(step, marks, *refs):
    peers, begin, forward, share, finish = _gather_plan(*refs)

    @pl.when(step == 0)
    def _():
        bar = pltpu.get_barrier_semaphore()
        for to in peers:
            pl.semaphore_signal(bar, inc=1, device_id={"tp": to}, device_id_type=MESH)
        pl.semaphore_wait(bar, 3)
        begin()

    pl.when(step == marks[0])(forward)
    pl.when(step == marks[1])(share)
    return finish


def _gather_all(*refs):
    for stage in _gather_plan(*refs)[1:]:
        stage()


def _mm(body, grid, ins, in_specs, outs, out_specs, flops, name, shard=None, cid=0, marks=(0, 0)):
    n_in, n_out = len(ins), len(outs)
    steps = grid[0] * grid[1]

    def plain(*refs):
        body(refs[:n_in], refs[n_in:])

    def comm(*refs):
        sh, out = refs[n_in], refs[n_in + 1 + n_out]
        step = pl.program_id(0) * grid[1] + pl.program_id(1)
        finish = _gather_events(step, marks, sh, out, *refs[n_in + n_out + 2:])
        body(refs[:n_in], refs[n_in + 1:n_in + 1 + n_out])
        pl.when(step == steps - 1)(finish)

    nbytes = sum(v.size * v.dtype.itemsize for v in ins) + sum(v.size * v.dtype.itemsize for v in outs)
    cost = pl.CostEstimate(flops=flops, bytes_accessed=nbytes, transcendentals=0)
    if shard is None:
        res = pl.pallas_call(plain, grid=grid, in_specs=in_specs, out_specs=out_specs, out_shape=outs, cost_estimate=cost,
                              compiler_params=pltpu.CompilerParams(vmem_limit_bytes=VMEM), name=name)(*ins)
        return res[0] if n_out == 1 else res
    any_spec = pl.BlockSpec(memory_space=pl.ANY)
    full = jax.ShapeDtypeStruct((shard.shape[0] * lax.axis_size("tp"), shard.shape[1]), shard.dtype)
    return pl.pallas_call(
        comm, grid=grid, in_specs=in_specs + [any_spec], out_specs=out_specs + [any_spec], out_shape=outs + [full],
        scratch_shapes=[pltpu.SemaphoreType.DMA, pltpu.SemaphoreType.DMA((10,)), pltpu.SemaphoreType.DMA((10,))],
        cost_estimate=cost, name=name,
        compiler_params=pltpu.CompilerParams(vmem_limit_bytes=VMEM, collective_id=cid, has_side_effects=True))(*ins, shard)


def _matmul(a, b, tb, bm, bn, name, dtype=BF, **kw):
    m, k = a.shape
    n = b.shape[0] if tb else b.shape[1]

    def body(i, o):
        o[0][...] = _dot(i[0][...], i[1][...], False, tb).astype(dtype)

    return _mm(body, (m // bm, n // bn), [a, b],
               [pl.BlockSpec((bm, k), lambda i, j: (i, 0)),
                pl.BlockSpec((bn, k), lambda i, j: (j, 0)) if tb else pl.BlockSpec((k, bn), lambda i, j: (0, j))],
               [jax.ShapeDtypeStruct((m, n), dtype)], [pl.BlockSpec((bm, bn), lambda i, j: (i, j))],
               2 * m * n * k, name, **kw)


def _mlp_up(n2, dg, w, lo, part=0, parts=1, prev=(), bn=512, sub=256):
    m, k = n2.shape
    n = w.shape[1]
    bm = m // parts
    off = lo // bm + part

    def body(n2_ref, w_ref, dg_ref, *rest):
        gb_ref, da_ref = rest[-2:]

        def finish(s, a):
            sl = slice(s, s + sub)
            a2 = a * a
            th = jnp.tanh(a * (C0 + (C0 * C1) * a2))
            p1 = 0.5 + 0.5 * th
            gb_ref[:, sl] = (a * p1).astype(BF)
            der = p1 + (a - a * (th * th)) * (0.5 * C0 + (1.5 * C0 * C1) * a2)
            da_ref[:, sl] = (dg_ref[:, sl] * der).astype(BF)

        held = None
        for s in range(0, bn, sub):
            a = _nn(n2_ref[...], w_ref[:, s:s + sub])
            if held is not None:
                finish(*held)
            held = (s, a)
        finish(*held)

    tile = pl.BlockSpec((bm, bn), lambda j: (part, j))
    return pl.pallas_call(
        body, grid=(n // bn,),
        in_specs=[pl.BlockSpec((bm, k), lambda j: (part, 0)), pl.BlockSpec((k, bn), lambda j: (0, j)),
                  pl.BlockSpec((bm, bn), lambda j: (off, j))] + [pl.BlockSpec(memory_space=pl.ANY)] * len(prev),
        out_specs=[tile, tile], out_shape=[jax.ShapeDtypeStruct((m, n), BF)] * 2,
        input_output_aliases={3: 0, 4: 1} if prev else {},
        cost_estimate=pl.CostEstimate(flops=2 * bm * n * k, bytes_accessed=2 * (bm * k + k * n) + 8 * bm * n, transcendentals=bm * n),
        compiler_params=pltpu.CompilerParams(vmem_limit_bytes=VMEM), name="mlp_up")(n2, w, dg, *prev)


def _wgrad(lhs, rhs, bm, bn, name, **kw):
    rows = min(v.shape[0] for v in lhs + rhs)

    def pieces(vs, width, pick):
        arrays, specs = [], []
        for v in vs:
            for p in range(v.shape[0] // rows):
                arrays.append(v)
                specs.append(pl.BlockSpec((rows, width), functools.partial(lambda p, i, j: (p, pick(i, j)), p)))
        return arrays, specs

    la, ls = pieces(lhs, bm, lambda i, j: i)
    ra, rs = pieces(rhs, bn, lambda i, j: j)
    n = len(la)
    m, w = lhs[0].shape[1], rhs[0].shape[1]

    def body(i, o):
        acc = _dot(i[0][...], i[n][...], True, False)
        for e in range(1, n):
            acc += _dot(i[e][...], i[n + e][...], True, False)
        o[0][...] = acc.astype(BF)

    return _mm(body, (m // bm, w // bn), la + ra, ls + rs, [jax.ShapeDtypeStruct((m, w), BF)],
               [pl.BlockSpec((bm, bn), lambda i, j: (i, j))], 2 * m * w * rows * n, name, **kw)


def _turn(part, xh, rs, g, skip, other, lhs, rhs, bm, bn, cid):
    tp = lax.axis_size("tp")
    chips = tp // 2
    t, d = part.shape
    sr = t // tp
    h = sr // 2
    n = len(lhs)
    rows = lhs[0].shape[0]
    m, w = lhs[0].shape[1], rhs[0].shape[1]
    grid = (m // bm, w // bn)
    steps = grid[0] * grid[1]
    arrays, specs = [], []
    for vs, width, pick in ((lhs, bm, lambda i, j: i), (rhs, bn, lambda i, j: j)):
        for v in vs:
            for p in range(v.shape[0] // rows):
                arrays.append(v)
                specs.append(pl.BlockSpec((rows, width), functools.partial(lambda pick, p, i, j: (p, pick(i, j)), pick, p)))
    n = len(arrays) // 2

    def kernel(*refs):
        ins, refs = refs[:2 * n], refs[2 * n:]
        part_ref, xh_ref, rs_ref, g_ref, skip_ref, refs = *refs[:5], refs[5:]
        other_in, (dw_ref, dh_ref, dh0_ref, dhb0_ref, full), refs = refs[:4], refs[4:9], refs[9:]
        own, mates, sums, fromleft, fromright, l1, r1, shard, lsem, asem, bsem, csem, dsem, gl, gs, gr = refs
        me = lax.axis_index("tp")
        chip, core = me // 2, lax.rem(me, 2)
        step = pl.program_id(0) * grid[1] + pl.program_id(1)
        order = [lax.rem(chip + e, chips) for e in (2, 1, chips - 1, 0)]
        right, left, mate = order[1] * 2 + core, order[2] * 2 + core, chip * 2 + 1 - core

        def block(c, k):
            return part_ref.at[pl.ds(pl.multiple_of((2 * c + k) * sr, 8), sr)]

        def remote(src, dst, ssem, rsem, to):
            return pltpu.make_async_remote_copy(src_ref=src, dst_ref=dst, send_sem=ssem, recv_sem=rsem,
                                                device_id={"tp": to}, device_id_type=MESH)

        loads = [pltpu.make_async_copy(block(order[e], core), own.at[e], lsem.at[e]) for e in range(4)]
        swaps = [remote(block(order[e], 1 - core), mates.at[e], asem.at[e], bsem.at[e], mate) for e in range(4)]
        lo, hi = pl.ds(0, h), pl.ds(h, h)
        legs = [(sums.at[0, lo], l1, right), (sums.at[0, hi], r1, left),
                (sums.at[1, hi], fromleft.at[hi], right), (sums.at[2, lo], fromright.at[lo], left),
                (sums.at[1, lo], fromleft.at[lo], right), (sums.at[2, hi], fromright.at[hi], left)]
        hops = [remote(src, dst, csem.at[e], dsem.at[e], to) for e, (src, dst, to) in enumerate(legs)]

        def pair(e, sl):
            return own[e, sl].astype(F32) + mates[e, sl].astype(F32)

        def ready(e):
            loads[e].wait()
            swaps[e].wait_recv()

        @pl.when(step == 0)
        def _():
            bar = pltpu.get_barrier_semaphore()
            for to in (left, right, mate):
                pl.semaphore_signal(bar, inc=1, device_id={"tp": to}, device_id_type=MESH)
            pl.semaphore_wait(bar, 3)
            for e in range(4):
                loads[e].start()
                swaps[e].start()

        @pl.when(step == 1)
        def _():
            ready(0)
            sums[0] = pair(0, pl.ds(0, sr)).astype(BF)
            hops[0].start()
            hops[1].start()
            ready(1)
            ready(2)
            sums[1, hi] = pair(1, hi).astype(BF)
            hops[2].start()
            sums[2, lo] = pair(2, lo).astype(BF)
            hops[3].start()

        @pl.when(step == 4)
        def _():
            hops[0].wait_recv()
            sums[1, lo] = (pair(1, lo) + l1[...].astype(F32)).astype(BF)
            hops[4].start()
            hops[1].wait_recv()
            sums[2, hi] = (pair(2, hi) + r1[...].astype(F32)).astype(BF)
            hops[5].start()
            red0, xh0, rs0, skip0 = other_in
            v0 = skip0[...].astype(F32) + _ln_bwd(red0[...].astype(F32), xh0[...], rs0[...], g_ref[...])
            dh0_ref[...] = v0
            dhb0_ref[...] = v0.astype(BF)

        acc = _dot(ins[0][...], ins[n][...], True, False)
        for e in range(1, n):
            acc += _dot(ins[e][...], ins[n + e][...], True, False)
        dw_ref[...] = acc.astype(BF)

        @pl.when(step == steps - 1)
        def _():
            ready(3)
            for e in (2, 3, 4, 5):
                hops[e].wait_recv()
            total = pair(3, pl.ds(0, sr)) + fromleft[...].astype(F32) + fromright[...].astype(F32)
            v = skip_ref[...].astype(F32) + _ln_bwd(total.astype(BF).astype(F32), xh_ref[...], rs_ref[...], g_ref[...])
            dh_ref[...] = v
            shard[...] = v.astype(BF)
            for cp in swaps:
                cp.wait_send()
            for cp in hops:
                cp.wait_send()
            _gather_all(shard, full, gl, gs, gr)

    one = lambda shape: pl.BlockSpec(shape, lambda i, j: (0, 0), pipeline_mode=pl.Buffered(1))
    res = pl.BlockSpec((sr, d), lambda i, j: (0, 0))
    any_spec = pl.BlockSpec(memory_space=pl.ANY)
    blk = pltpu.VMEM((sr, d), BF)
    sem = pltpu.SemaphoreType.DMA
    return pl.pallas_call(
        kernel, grid=grid,
        in_specs=specs + [any_spec, one((sr, d)), one((sr, 1)), one((1, d)), one((sr, d)),
                          one((sr, d)), one((sr, d)), one((sr, 1)), one((sr, d))],
        out_specs=[pl.BlockSpec((bm, bn), lambda i, j: (i, j)), res, res, res, any_spec],
        out_shape=[jax.ShapeDtypeStruct((m, w), BF), jax.ShapeDtypeStruct((sr, d), F32), jax.ShapeDtypeStruct((sr, d), F32),
                   jax.ShapeDtypeStruct((sr, d), BF), jax.ShapeDtypeStruct((t, d), BF)],
        scratch_shapes=[pltpu.VMEM((4, sr, d), BF), pltpu.VMEM((4, sr, d), BF), pltpu.VMEM((3, sr, d), BF), blk, blk,
                        pltpu.VMEM((h, d), BF), pltpu.VMEM((h, d), BF), blk,
                        sem((4,)), sem((4,)), sem((4,)), sem((6,)), sem((6,)), sem, sem((10,)), sem((10,))],
        cost_estimate=pl.CostEstimate(flops=4 * m * w * rows * n, bytes_accessed=64 * 2 ** 20, transcendentals=0),
        compiler_params=pltpu.CompilerParams(vmem_limit_bytes=VMEM, collective_id=cid, has_side_effects=True),
        name="turn")(*arrays, part, xh, rs, g, skip, *other)


def _rowwise(body, ins, outs, name, slot=0, prev=()):
    sr = ins[0].shape[0]
    grid = sr // ROWS

    def spec(v):
        if len(v.shape) > 2:
            return pl.BlockSpec((None, ROWS, v.shape[-1]), lambda i: (slot, i, 0))
        return pl.BlockSpec((ROWS, v.shape[1]), lambda i: (i, 0)) if v.shape[0] == sr else pl.BlockSpec(v.shape, lambda i: (0, 0))

    return pl.pallas_call(body, grid=(grid,), in_specs=[spec(v) for v in ins] + [pl.BlockSpec(memory_space=pl.ANY)] * len(prev),
                          out_specs=[spec(v) for v in outs], out_shape=outs,
                          input_output_aliases={len(ins): 0} if prev else {},
                          compiler_params=pltpu.CompilerParams(vmem_limit_bytes=VMEM), name=name)(*ins, *prev)


def _norm_kernel(red, x, g, n_ref, xh_ref, rs_ref):
    h1 = x[...].astype(F32) + red[...].astype(F32)
    xc = h1 - _mean(h1)
    rs = lax.rsqrt(_mean(xc * xc) + EPS)
    xh_ref[...] = xc * rs
    rs_ref[...] = rs
    n_ref[...] = (xh_ref[...] * g[...]).astype(BF)


def _dx_kernel(red, x, mu, rs, g, dh, *refs):
    xh = (x[...].astype(F32) - mu[...]) * rs[...]
    refs[-1][...] = (dh[...] + _ln_bwd(red[...].astype(F32), xh, rs[...], g[...])).astype(BF)


def _relay_kernel(i, o):
    o[...] = i[...]


def _relay(v):
    spec = pl.BlockSpec((v.shape[0] // 8, v.shape[1]), lambda i: (i, 0))
    return pl.pallas_call(_relay_kernel, grid=(8,), in_specs=[spec], out_specs=spec, out_shape=jax.ShapeDtypeStruct(v.shape, v.dtype),
                          cost_estimate=pl.CostEstimate(flops=v.size * v.shape[1], bytes_accessed=v.size, transcendentals=0),
                          compiler_params=pltpu.CompilerParams(vmem_limit_bytes=VMEM), name="relay")(v)


def solution(mesh):
    tp = mesh.shape["tp"]

    def body(x, mu1, rs1, g1, g2, dy, wqkv, wo, w1, w2):
        hl, hd, d = wo.shape
        t = x.shape[0]
        ct = t // NC
        sh = ct // tp
        me = lax.axis_index("tp")
        wo2 = wo.reshape(hl * hd, d)
        g1f = g1.astype(F32)
        g2f = g2.astype(F32)
        mur, rsr, g1r = mu1[None, :], rs1[None, :], g1f[None, :]

        def rows(v, c):
            return lax.dynamic_slice_in_dim(v, c * ct + me * sh, sh, 0)

        def rscat(v):
            return lax.psum_scatter(v, "tp", scatter_dimension=0, tiled=True)

        def gather(v):
            return lax.all_gather(v, "tp", axis=0, tiled=True)

        def after(v, dep):
            return lax.optimization_barrier((v, dep))[0]

        def ln2(c, red):
            shard = jax.ShapeDtypeStruct(red.shape, F32)
            outs = [jax.ShapeDtypeStruct(red.shape, BF), shard, jax.ShapeDtypeStruct((sh, 1), F32)]
            return _rowwise(_norm_kernel, [red, xrows[c], g2f[None, :]], outs, "norm2")

        def fwd(c, x):
            n1, qkv = _norm_qkv(x, mur, rsr, g1r, wqkv, c * ct, ct)
            qkvs.append(qkv)
            n1s.append(n1)
            os.append(_attn_fwd(c, qkvs, hl, hd))
            return _matmul(os[c], wo2, False, ct, 1024, "attn_out")

        xrows = [rows(x, c) for c in range(NC)]
        n1s, qkvs, os = [], [], []
        p0 = fwd(0, x)
        r0 = rscat(p0)
        p1 = fwd(1, after(x, p0))
        r1 = rscat(p1)
        n2a, xh2a, rs2a = ln2(0, after(r0, p1))
        dg, n2_0 = _matmul(dy, w2, True, 1024, 512, "dgate", F32, shard=n2a, cid=0, marks=(3, 5))
        half = _mlp_up(n2_0, dg, w1, 0, 0, 2)
        n2b, xh2b, rs2b = ln2(1, after(r1, half[0]))
        n2_1 = gather(n2b)
        gb0, da0 = _mlp_up(after(n2_0, n2b), dg, w1, 0, 1, 2, half)
        q0 = _matmul(da0, w1, True, ct, 512, "mlp_back")
        s0 = rscat(q0)
        gb1, da1 = _mlp_up(after(n2_1, q0), dg, w1, ct)
        q1 = _matmul(da1, w1, True, ct, 512, "mlp_back")
        dw2, dh1b, dh1a, dha, dh1_1 = _turn(q1, xh2b, rs2b, g2f[None, :], rows(dy, 1), (s0, xh2a, rs2a, rows(dy, 0)),
                                            [gb0, gb1], [dy], 1024, 1024, 1)
        dh1_0 = gather(dha)

        def bwd(c, dh, prev):
            do = _matmul(dh, wo2, True, 512, hl * hd, "dattn_out")
            dqkv, prev = _attn_bwd(c, NC, qkvs, do, prev, hl, hd)
            return dqkv, prev, _matmul(dqkv, wqkv, True, ct, 1024, "qkv_back")

        dqkv1, prev, u1 = bwd(1, dh1_1, [])
        v1 = rscat(u1)
        dqkv0, prev, u0 = bwd(0, after(dh1_0, u1), prev)
        v0 = rscat(u0)

        def dln1(c, red, dh1, *prev):
            ins = [red, xrows[c], rows(mu1, c)[:, None], rows(rs1, c)[:, None], g1r, dh1]
            return _rowwise(_dx_kernel, ins, [jax.ShapeDtypeStruct((NC, sh, d), BF)], "dx", c, prev)[0]

        dwqkv = _wgrad(n1s, [after(dqkv0, u0), dqkv1], 1024, dqkv0.shape[1] // 2, "dwqkv")
        dxb = dln1(1, after(v1, dwqkv), dh1b)
        dwo = _wgrad([after(os[0], dxb), os[1]], [dh1_0, dh1_1], hl * hd, 1024, "dwo")
        dxa = dln1(0, after(v0, dwo), dh1a, dxb)
        dx = lax.all_gather(dxa, "tp", axis=1, tiled=True).reshape(t, d)
        dw1 = _wgrad([n2_0, n2_1], [da0, after(da1, dxa)], 1024, 1024, "dw1")
        dw2 = _relay(after(dw2, dw1))
        return dx, dwqkv, dwo.reshape(hl, hd, d), dw1, dw2

    return jax.shard_map(
        body, mesh=mesh,
        in_specs=(P("dp", None), P("dp"), P("dp"), P(None), P(None), P("dp", None),
                  P(None, "tp"), P("tp", None, None), P(None, "tp"), P("tp", None)),
        out_specs=(P("dp", None), P("dp", "tp"), P(("dp", "tp"), None, None), P("dp", "tp"), P(("dp", "tp"), None)),
        check_vma=False)
```
